32 devices in a mesh: ctx: 8 (over y, x, core), fsdp: 4 (over z).
Axes of the slice: x: 2, y: 2, z: 4, core: 2. Of those that a mesh axis runs over, the one named last changes fastest.
Arguments:
- inputs: bfloat16 [4, 1024, 1536], P('fsdp', 'ctx')
- positions: int32 [4, 1024], P('fsdp', 'ctx'), may hold values from 0 to 1535, as said below
- block_order: int32 [16], replicated, may hold values from 0 to 15, as said below
- attention_gain: bfloat16 [1536], P('fsdp'), may hold values from 0.5 to 1.5
- projection: bfloat16 [1536, 2048], P('fsdp')
- projection_bias: bfloat16 [2048], P('fsdp'), may hold values from -4 to 4
- output_weight: bfloat16 [1536, 1536], P('fsdp'), may hold values from -1.5 to 1.5
- feedforward_gain: bfloat16 [1536], P('fsdp'), may hold values from 0.5 to 1.5
- gate_up: bfloat16 [1536, 17920], P('fsdp'), may hold values from -0.15625 to 0.15625
- down_weight: bfloat16 [8960, 1536], P('fsdp'), may hold values from -0.0625 to 0.0625
- cotangent: bfloat16 [4, 1024, 1536], P('fsdp', 'ctx'), may hold values from -6 to 6
Outputs:
- outputs: bfloat16 [4, 1024, 1536], P('fsdp', 'ctx')
- gradient: bfloat16 [4, 1024, 1536], P('fsdp', 'ctx')
- gradient_attention_gain: float32 [1536], P(('ctx', 'fsdp'))
- gradient_projection: float32 [1536, 2048], P('fsdp', 'ctx')
- gradient_projection_bias: float32 [2048], P(('ctx', 'fsdp'))
- gradient_output: float32 [1536, 1536], P('fsdp', 'ctx')
- gradient_feedforward_gain: float32 [1536], P(('ctx', 'fsdp'))
- gradient_gate_up: float32 [1536, 17920], P('fsdp', 'ctx')
- gradient_down: float32 [8960, 1536], P('fsdp', 'ctx')
The draws below stay inside these ranges and needn't reach their ends.
Inputs may be any that keep to these rules, and one draw needn't show every extreme that they name: `block_order`: A permutation: each of 0 to 15 appears once. Within each sequence, positions grow strictly with order_index; the sequence's first token has position 0, and of the 1023 steps between tokens next to each other in the sequence exactly 512 are 2 and the others are 1, so the last token has position 1535.
All inputs are finite; a program needn't handle non-finite values.
Results may differ from the reference program's by a relative error of at most 0.02.
Values may be sent and summed in bfloat16 or wider, within the bound.
A program may use at most 320 MiB of HBM per device.

```python
import math
import jax
import jax.numpy as jnp
from jax import lax

D = 1536
HEADS = 12
KV_HEADS = 2
HEAD = 128
FF = 8960
HALF = 64
BLOCKS = 16
LEN = 1024
SEQS = 4
QKV = 2048


def draw_inputs(key, part):
    base = jax.random.truncated_normal(jax.random.fold_in(key, 1), -6.0, 6.0, (SEQS, LEN, D), jnp.float32)
    return base.astype(jnp.bfloat16)


def draw_projection(key, part):
    base = jax.random.truncated_normal(jax.random.fold_in(key, 21), -6.0, 6.0, (D, QKV), jnp.float32) / math.sqrt(D)
    return base.astype(jnp.bfloat16)


def draw_block_order(key, part):
    return jax.random.permutation(jax.random.fold_in(key, 5), BLOCKS).astype(jnp.int32)


def draw_positions(key, part):
    order = jax.random.permutation(jax.random.fold_in(key, 5), BLOCKS)
    steps = jnp.where(jnp.arange(LEN - 1) < LEN // 2, 2, 1).astype(jnp.int32)
    steps = jnp.broadcast_to(steps[None, :], (SEQS, LEN - 1))
    steps = jax.random.permutation(jax.random.fold_in(key, 6), steps, axis=1, independent=True)
    places = jnp.concatenate([jnp.zeros((SEQS, 1), jnp.int32), jnp.cumsum(steps, axis=1).astype(jnp.int32)], axis=1)
    arranged = places.reshape(SEQS, BLOCKS, HALF)[:, order, :]
    return arranged.reshape(SEQS, LEN).astype(jnp.int32)


def shard_levels(stream_key, shape, pieces, least, high):
    def one(axis_at, blocks):
        steps = jax.random.uniform(jax.random.fold_in(jax.random.fold_in(stream_key, 6), axis_at), (blocks,), jnp.float32, least / len(pieces), high / len(pieces))
        return jnp.repeat(jnp.exp(steps), shape[axis_at] // blocks).reshape((-1,) + (1,) * (len(shape) - axis_at - 1))

    gain = one(*pieces[0])
    for cut in pieces[1:]:
        gain = gain * one(*cut)
    return gain


def centred(stream_key, dims, scale, limit, shards=(), held_as=jnp.bfloat16):
    factor_of = shard_levels(stream_key, dims, shards, -0.22, 0.18) if shards else 1.0
    drawn = jax.random.normal(stream_key, dims, jnp.float32) * scale * factor_of
    return jnp.minimum(jnp.maximum(drawn, -limit), limit).astype(held_as)


def setup_inputs(seed: int = 0) -> dict:
    arg_keys = jax.random.split(jax.random.key(seed), 12)
    inputs = draw_inputs(jax.random.fold_in(arg_keys[11], 71), 0)
    positions = draw_positions(jax.random.fold_in(arg_keys[11], 71), 0)
    block_order = draw_block_order(jax.random.fold_in(arg_keys[11], 71), 0)
    attention_gain = jnp.clip(1.0 + 0.1 * jax.random.normal(arg_keys[3], (D,), jnp.float32), 0.5, 1.5).astype(jnp.bfloat16)
    projection = draw_projection(jax.random.fold_in(arg_keys[11], 71), 0)
    projection_bias = centred(arg_keys[5], (QKV,), 1.0, 4.0, ((0, 4),))
    output_weight = centred(arg_keys[6], (HEADS * HEAD, D), 16 ** -0.5, 1.5, ((0, 4),))
    feedforward_gain = jnp.clip(1.0 + 0.1 * jax.random.normal(arg_keys[7], (D,), jnp.float32), 0.5, 1.5).astype(jnp.bfloat16)
    gate_up = centred(arg_keys[8], (D, 2 * FF), D ** -0.5, 0.15625, ((0, 4),))
    down_weight = centred(arg_keys[9], (FF, D), FF ** -0.5, 0.0625, ((0, 4),))
    cotangent = centred(arg_keys[10], (SEQS, LEN, D), 1.0, 6.0, ((0, 4), (1, 8)))
    return {"inputs": inputs, "positions": positions, "block_order": block_order, "attention_gain": attention_gain, "projection": projection, "projection_bias": projection_bias, "output_weight": output_weight, "feedforward_gain": feedforward_gain, "gate_up": gate_up, "down_weight": down_weight, "cotangent": cotangent}


EPS = 1e-06
THETA = 1000000.0
NEGATIVE = -1e+30
HIGHEST = lax.Precision.HIGHEST

@jax.custom_vjp
def low(v):
    return lax.optimization_barrier(v.astype(jnp.bfloat16)).astype(jnp.float32)

@jax.custom_vjp
def low_back(v):
    return v

def low_keep(v):
    return (low(v), None)

def low_pass(kept, grad):
    return (grad,)

def back_keep(v):
    return (v, None)

def back_low(kept, grad):
    return (low(grad),)
low.defvjp(low_keep, low_pass)
low_back.defvjp(back_keep, back_low)

def rope_tables(places):
    freq = THETA ** (-jnp.arange(0, HEAD, 2).astype(jnp.float32) / HEAD)
    angle = places.astype(jnp.float32)[:, None] * freq[None, :]
    angle = jnp.concatenate([angle, angle], axis=-1)
    return (jnp.cos(angle), jnp.sin(angle))

def rotate(values):
    middle = values.shape[-1] // 2
    return jnp.concatenate([-values[..., middle:], values[..., :middle]], axis=-1)

def apply_rope(values, cosine, sine):
    return values * cosine[:, None, :] + rotate(values) * sine[:, None, :]

def layer(parameters, features, cosine, sine, order_index):
    gain_one, projection, bias, output_weight, gain_two, gate_up, down_weight = parameters
    length = features.shape[0]
    query_width = HEADS * HEAD
    key_width = KV_HEADS * HEAD
    ratio = HEADS // KV_HEADS
    inverse_one = lax.rsqrt(lax.optimization_barrier(jnp.mean(features * features, axis=-1, keepdims=True)) + EPS)
    normed_one = low(features * inverse_one * gain_one)
    projected = low_back(jnp.dot(normed_one, projection, precision=HIGHEST) + bias)
    queries = low(apply_rope(projected[:, :query_width].reshape(length, HEADS, HEAD), cosine, sine))
    keys = low(apply_rope(projected[:, query_width:query_width + key_width].reshape(length, KV_HEADS, HEAD), cosine, sine))
    values = low(projected[:, query_width + key_width:].reshape(length, KV_HEADS, HEAD))
    grouped = queries.reshape(length, KV_HEADS, ratio, HEAD)
    block = math.gcd(length, 512)

    def attend(item):
        query_block, index_block = item
        scores = jnp.einsum('qgrd,kgd->gqrk', query_block, keys, precision=HIGHEST) * (1.0 / math.sqrt(HEAD))
        scores = low_back(scores)
        mask = order_index[None, :] <= index_block[:, None]
        scores = jnp.where(mask[None, :, None, :], scores, NEGATIVE)
        probs = low(jax.nn.softmax(scores, axis=-1))
        return jnp.einsum('gqrk,kgd->qgrd', probs, values, precision=HIGHEST)
    attention = lax.map(jax.checkpoint(attend), (grouped.reshape(length // block, block, KV_HEADS, ratio, HEAD), order_index.reshape(length // block, block)))
    merged = low(low_back(attention.reshape(length, query_width)))
    branch = low_back(jnp.dot(merged, output_weight, precision=HIGHEST))
    residual = features + branch
    inverse_two = lax.rsqrt(lax.optimization_barrier(jnp.mean(residual * residual, axis=-1, keepdims=True)) + EPS)
    normed_two = low(residual * inverse_two * gain_two)
    gate_values = low_back(jnp.dot(normed_two, gate_up, precision=HIGHEST))
    gate = gate_values[:, :FF]
    upward = gate_values[:, FF:]
    activation = low(jax.nn.silu(gate) * upward)
    return residual + jnp.dot(activation, down_weight, precision=HIGHEST)

def reference(inputs, positions, block_order, attention_gain, projection, projection_bias, output_weight, feedforward_gain, gate_up, down_weight, cotangent):
    parameters = tuple((item.astype(jnp.float32) for item in (attention_gain, projection, projection_bias, output_weight, feedforward_gain, gate_up, down_weight)))
    slots = jnp.arange(LEN, dtype=jnp.int32)
    order_index = (block_order[slots // HALF] * HALF + slots % HALF).astype(jnp.int32)

    def one_sequence(totals, item):
        features, places, tangent = item
        cosine, sine = rope_tables(places)

        def forward(params, values):
            return layer(params, values, cosine, sine, order_index)
        result, pullback = jax.vjp(forward, parameters, features.astype(jnp.float32))
        grads, d_features = pullback(tangent.astype(jnp.float32))
        totals = jax.tree.map(lambda left, right: left + right, totals, grads)
        return (totals, (result.astype(jnp.bfloat16), d_features.astype(jnp.bfloat16)))
    start = jax.tree.map(jnp.zeros_like, parameters)
    totals, (outputs, gradient) = lax.scan(one_sequence, start, (inputs, positions, cotangent))
    return (outputs, gradient, totals[0], totals[1], totals[2], totals[3], totals[4], totals[5], totals[6])
```

```python
import math

import jax
import jax.numpy as jnp
from jax import lax
from jax.sharding import PartitionSpec as P

HEADS = 12
KV_HEADS = 2
HEAD = 128
FF = 8960
GROUP = 2

EPS = 1e-06
THETA = 1000000.0
NEGATIVE = -1e30
BF = jnp.bfloat16
F32 = jnp.float32


def rope_tables(places):
    freq = THETA ** (-jnp.arange(0, HEAD, 2).astype(F32) / HEAD)
    angle = places.astype(F32)[:, None] * freq[None, :]
    angle = jnp.concatenate([angle, angle], axis=-1)
    return (jnp.cos(angle), jnp.sin(angle))


def rotate(values):
    middle = values.shape[-1] // 2
    return jnp.concatenate([-values[..., middle:], values[..., :middle]], axis=-1)


def apply_rope(values, cosine, sine):
    return values * cosine[:, None, :] + rotate(values) * sine[:, None, :]


def rope_back(grads, cosine, sine):
    return grads * cosine[:, None, :] - rotate(grads * sine[:, None, :])


def order_rows(block_order, start, count, half):
    offsets = start + jnp.arange(count, dtype=jnp.int32)
    slots = offsets // half
    table = jnp.arange(block_order.shape[0], dtype=jnp.int32)
    picked = jnp.sum(jnp.where(slots[:, None] == table[None, :], block_order[None, :], 0), axis=1)
    return picked * half + offsets % half


def rms_inverse(values):
    return lax.rsqrt(jnp.mean(values * values, axis=-1, keepdims=True) + EPS)


def norm_back(d_normed, values, inverse, gain):
    unit = values * inverse
    d_unit = d_normed * gain
    d_gain = jnp.sum(d_normed * unit, axis=0)
    d_values = inverse * (d_unit - unit * jnp.mean(d_unit * unit, axis=-1, keepdims=True))
    return (d_values, d_gain)


def dot(left, right, dims, out=F32):
    return lax.dot_general(left, right, (dims, ((), ())), preferred_element_type=out)


def swapped(x, size):
    return lax.ppermute(x, "fsdp", [(i, i ^ 1) for i in range(size)])


def gather_tokens(x, size):
    both = jnp.stack([x, swapped(x, size)])
    return lax.all_gather(both, "ctx", axis=1, tiled=True)


def scatter_tokens(partial, size):
    parts = lax.psum_scatter(partial, "ctx", scatter_dimension=1, tiled=True)
    return parts[0].astype(F32) + swapped(parts[1], size).astype(F32)


def body(
    inputs,
    positions,
    block_order,
    attention_gain,
    projection,
    projection_bias,
    output_weight,
    feedforward_gain,
    gate_up,
    down_weight,
    cotangent,
):
    rows, width = inputs.shape[1:]
    half = rows // 2
    ratio = HEADS // KV_HEADS
    query_width = HEADS * HEAD
    key_width = KV_HEADS * HEAD
    cycle = lax.axis_size("ctx")
    owners = lax.axis_size("fsdp")
    place = lax.axis_index("ctx")
    owner = lax.axis_index("fsdp")
    fold = owners // GROUP
    unit = FF // (owners * cycle)
    depth = width // owners
    length = rows * cycle

    slab = depth // cycle
    whole_projection = lax.all_gather(
        lax.dynamic_slice_in_dim(projection, place * slab, slab, 0), ("fsdp", "ctx"), axis=0, tiled=True
    )
    whole_output = lax.all_gather(
        lax.dynamic_slice_in_dim(output_weight, place * slab, slab, 0), ("fsdp", "ctx"), axis=0, tiled=True
    )
    small = lax.all_gather(
        jnp.concatenate([attention_gain, feedforward_gain, projection_bias]), "fsdp", axis=0
    )
    gain_one = small[:, :depth].reshape(-1).astype(F32)
    gain_two = small[:, depth : 2 * depth].reshape(-1).astype(F32)
    bias = small[:, 2 * depth :].reshape(-1).astype(F32)

    pieces = []
    for side in range(2):
        for plane in range(owners):
            start = side * FF + plane * (FF // owners) + place * unit
            pieces.append(lax.dynamic_slice_in_dim(gate_up, start, unit, 1))

    def part(side, to):
        return jnp.concatenate(
            [pieces[side * owners + (to + GROUP * b) % owners] for b in range(fold)], axis=1
        )

    sent = jnp.stack([jnp.stack([part(side, to) for side in range(2)]) for to in range(owners)])
    got = lax.all_to_all(sent, "fsdp", split_axis=0, concat_axis=0, tiled=True)
    gate_weight = got[:, 0].reshape(width, fold * unit)
    up_weight = got[:, 1].reshape(width, fold * unit)
    own_down = lax.dynamic_slice_in_dim(down_weight, place * unit, unit, 0)
    down = [own_down]
    for b in range(1, fold):
        route = [((i + GROUP * b) % owners, i) for i in range(owners)]
        down.append(lax.ppermute(own_down, "fsdp", route))
    down = jnp.concatenate(down, axis=0)

    tangent = cotangent[0]
    tangents = gather_tokens(tangent, owners).reshape(GROUP * length, width)

    features = inputs[0].astype(F32)
    inverse_one = rms_inverse(features)
    normed_one = (features * inverse_one * gain_one).astype(BF)
    projected = dot(normed_one, whole_projection, ((1,), (0,))) + bias
    cosine, sine = rope_tables(positions[0])
    queries = apply_rope(projected[:, :query_width].reshape(rows, HEADS, HEAD), cosine, sine).astype(BF)
    keys = apply_rope(
        projected[:, query_width : query_width + key_width].reshape(rows, KV_HEADS, HEAD), cosine, sine
    ).astype(BF)
    values = projected[:, query_width + key_width :].astype(BF)
    pairs = lax.all_gather(
        jnp.concatenate([keys.reshape(rows, key_width), values], axis=1), "ctx", axis=0, tiled=True
    )
    all_keys = pairs[:, :key_width].reshape(length, KV_HEADS, HEAD)
    all_values = pairs[:, key_width:].reshape(length, KV_HEADS, HEAD)
    grouped = queries.reshape(rows, KV_HEADS, ratio, HEAD).transpose(1, 2, 0, 3)
    own_index = order_rows(block_order, place * rows, rows, half)
    all_index = order_rows(block_order, 0, length, half)
    mask = (all_index[None, :] <= own_index[:, None])[None, None]
    scale = 1.0 / math.sqrt(HEAD)

    def weights_of():
        scores = jnp.einsum("grqd,kgd->grqk", grouped, all_keys, preferred_element_type=F32) * scale
        return jnp.where(mask, scores, NEGATIVE)

    scores = weights_of()
    top = jnp.max(scores, axis=-1, keepdims=True)
    probs = jnp.exp(scores - top)
    total = jnp.sum(probs, axis=-1, keepdims=True)
    probs = probs / total
    low_probs = probs.astype(BF)
    attention = jnp.einsum("grqk,kgd->grqd", low_probs, all_values, preferred_element_type=F32)
    merged = attention.transpose(2, 0, 1, 3).reshape(rows, query_width).astype(BF)
    residual = features + dot(merged, whole_output, ((1,), (0,)))
    inverse_two = rms_inverse(residual)
    normed_two = (residual * inverse_two * gain_two).astype(BF)

    tokens = gather_tokens(normed_two, owners).reshape(GROUP * length, width)
    gate = dot(tokens, gate_weight, ((1,), (0,)))
    upward = dot(tokens, up_weight, ((1,), (0,)))
    sigmoid = jax.nn.sigmoid(gate)
    activation = (gate * sigmoid * upward).astype(BF)
    branch = dot(activation, down, ((1,), (0,)), BF).reshape(GROUP, length, width)
    outputs = (residual + scatter_tokens(branch, owners)).astype(BF)
    d_activation = dot(tangents, down, ((1,), (1,)))
    d_gate = (d_activation * upward * sigmoid * (1.0 + gate * (1.0 - sigmoid))).astype(BF)
    d_upward = (d_activation * gate * sigmoid).astype(BF)
    d_tokens = (
        dot(d_gate, gate_weight, ((1,), (1,))) + dot(d_upward, up_weight, ((1,), (1,)))
    ).astype(BF)
    d_normed_two = scatter_tokens(d_tokens.reshape(GROUP, length, width), owners)
    grad_gate = dot(tokens, d_gate, ((0,), (0,)), BF)
    grad_up = dot(tokens, d_upward, ((0,), (0,)), BF)
    grad_down = dot(activation, tangents, ((0,), (0,)), BF)

    mine = lax.all_to_all(
        jnp.stack([grad_gate.reshape(owners, depth, -1), grad_up.reshape(owners, depth, -1)], 1),
        "fsdp", split_axis=0, concat_axis=0, tiled=True,
    )
    folded = []
    for plane in range(owners):
        total_piece = 0.0
        for source in range(plane % GROUP, owners, GROUP):
            b = ((plane - source) // GROUP) % fold
            total_piece = total_piece + mine[source, :, :, b * unit : (b + 1) * unit].astype(F32)
        folded.append(total_piece.astype(BF))
    folded = jnp.stack(folded, axis=1)
    spread = lax.all_to_all(
        folded.reshape(cycle, 2 * owners // cycle, depth, unit), "ctx", split_axis=0, concat_axis=0, tiled=True
    )
    final_gate_up = spread.transpose(2, 1, 0, 3).reshape(depth, -1).astype(F32)
    grad_down = grad_down.reshape(fold, unit, width)
    total_down = grad_down[0].astype(F32)
    for b in range(1, fold):
        route = [(i, (i + GROUP * b) % owners) for i in range(owners)]
        total_down = total_down + lax.ppermute(grad_down[b], "fsdp", route).astype(F32)
    final_down = lax.all_to_all(
        total_down.astype(BF).reshape(unit, cycle, width // cycle).transpose(1, 0, 2),
        "ctx", split_axis=0, concat_axis=0, tiled=True,
    ).reshape(-1, width // cycle).astype(F32)

    d_residual, grad_gain_two = norm_back(d_normed_two, residual, inverse_two, gain_two)
    d_residual = d_residual + tangent.astype(F32)
    d_branch = d_residual.astype(BF)
    d_merged = dot(d_branch, whole_output, ((1,), (1,))).astype(BF)
    d_attention = d_merged.reshape(rows, KV_HEADS, ratio, HEAD).transpose(1, 2, 0, 3)
    delta = jnp.sum(d_attention.astype(F32) * attention, axis=-1, keepdims=True)
    d_values = jnp.einsum("grqk,grqd->kgd", low_probs, d_attention, preferred_element_type=F32)
    d_probs = jnp.einsum("grqd,kgd->grqk", d_attention, all_values, preferred_element_type=F32)
    d_scores = (probs * (d_probs - delta)).astype(BF)
    d_queries = jnp.einsum("grqk,kgd->qgrd", d_scores, all_keys, preferred_element_type=F32) * scale
    d_keys = jnp.einsum("grqk,grqd->kgd", d_scores, grouped, preferred_element_type=F32) * scale
    d_pairs = jnp.concatenate(
        [d_keys.reshape(length, key_width), d_values.reshape(length, key_width)], axis=1
    ).astype(BF)
    d_pairs = lax.psum_scatter(d_pairs, "ctx", scatter_dimension=0, tiled=True).astype(F32)
    d_query_raw = rope_back(d_queries.reshape(rows, HEADS, HEAD), cosine, sine)
    d_key_raw = rope_back(d_pairs[:, :key_width].reshape(rows, KV_HEADS, HEAD), cosine, sine)
    d_projected = jnp.concatenate(
        [d_query_raw.reshape(rows, query_width), d_key_raw.reshape(rows, key_width), d_pairs[:, key_width:]],
        axis=1,
    ).astype(BF)
    grad_bias = jnp.sum(d_projected.astype(F32), axis=0)
    d_normed_one = dot(d_projected, whole_projection, ((1,), (1,)))
    d_features, grad_gain_one = norm_back(d_normed_one, features, inverse_one, gain_one)
    gradient = (d_residual + d_features).astype(BF)

    def columns_home(left, right):
        whole_left = lax.all_gather(left, "ctx", axis=0, tiled=True)
        share = right.shape[1] // cycle
        sliced = lax.all_to_all(
            right.reshape(rows, cycle, share).transpose(1, 0, 2), "ctx", split_axis=0, concat_axis=0, tiled=True
        ).reshape(length, share)
        partial = dot(whole_left, sliced, ((0,), (0,)), BF).reshape(owners, depth, share)
        parts = lax.all_to_all(partial, "fsdp", split_axis=0, concat_axis=0, tiled=True)
        return jnp.sum(parts.astype(F32), axis=0)

    final_output = columns_home(merged, d_branch)
    final_projection = columns_home(normed_one, d_projected)
    count = owners * cycle
    sums = jnp.concatenate(
        [grad_gain_one.reshape(count, -1), grad_bias.reshape(count, -1), grad_gain_two.reshape(count, -1)], axis=1
    )
    sums = lax.psum_scatter(sums, ("ctx", "fsdp"), scatter_dimension=0, tiled=True)[0]
    first = width // count
    last = sums.shape[0] - first
    return (
        outputs[None],
        gradient[None],
        sums[:first],
        final_projection,
        sums[first:last],
        final_output,
        sums[last:],
        final_gate_up,
        final_down,
    )


def solution(mesh):
    return jax.shard_map(
        body,
        mesh=mesh,
        in_specs=(
            P("fsdp", "ctx", None),
            P("fsdp", "ctx"),
            P(),
            P("fsdp"),
            P("fsdp", None),
            P("fsdp"),
            P("fsdp", None),
            P("fsdp"),
            P("fsdp", None),
            P("fsdp", None),
            P("fsdp", "ctx", None),
        ),
        out_specs=(
            P("fsdp", "ctx", None),
            P("fsdp", "ctx", None),
            P(("ctx", "fsdp")),
            P("fsdp", "ctx"),
            P(("ctx", "fsdp")),
            P("fsdp", "ctx"),
            P(("ctx", "fsdp")),
            P("fsdp", "ctx"),
            P("fsdp", "ctx"),
        ),
        check_vma=False,
    )
```
